128 devices in a mesh: row: 8 (over z, core), col: 16 (over x, y).
Axes of the slice: x: 4, y: 4, z: 4, core: 2. Of those that a mesh axis runs over, the one named last changes fastest.
Arguments:
- trial_factor: bfloat16 [2, 8192, 512], P(None, ('row', 'col')), may hold values from -6 to 6
- occupied: bfloat16 [8192, 512], P(('col', 'row')), may hold values from -0.25 to 0.25
- centers: float32 [3, 8192], P(None, ('row', 'col')), may hold values from 0 to 1
- exponents: float32 [8192], P(('row', 'col')), may hold values from 0.5 to 4
- wave_vectors: float32 [3, 8192], P(None, ('row', 'col')), may hold values from -36 to 36
- phases: float32 [8192], P(('row', 'col')), may hold values from -3.140625 to 3.140625
- points: float32 [256, 3, 1024], P(('row', 'col')), may hold values from 0 to 1
- density: float32 [256, 1024], P(('row', 'col')), may hold values from 0.05 to 1
- weights: float32 [256, 1024], P(('row', 'col')), may hold values from 0.0001 to 0.001
- sources: int32 [256, 8, 1], P(('row', 'col')), may hold values from 0 to 15; in each aligned block of 16 rows (0 to 15, 16 to 31, ..., all dimensions but the last counted through in order) at most 2 rows name the same one
Outputs:
- response: float32 [8192, 2, 512], P(('row', 'col'))
The draws below stay inside these ranges and needn't reach their ends.
Inputs may be any that keep to these rules, and one draw needn't show every extreme that they name: `sources`: among the 16 entries of the batches of one device, no column block is named more than 2 times, and some block exactly 2 times.
All inputs are finite; a program needn't handle non-finite values.
Results may differ from the reference program's by a relative error of at most 0.0065.
Values may be sent and summed in bfloat16 or wider, within the bound.
A program may use at most 128 MiB of HBM per device.

```python
import math
import jax
import jax.numpy as jnp
import numpy as np
from jax import lax

NOCC = 512
TB = 256
TR = 4
TC = 2
K = 2
BATCH_DEV = 2
GB = 1024
NPAIR = 8
COLS = 16
NBF = 8192
BATCHES = 256
CAP = 2
N_COL = 16


def block_scale(stream_key, dims, split, smallest, top_value):
    gain = 1.0
    for axis_at, parts in split:
        steps = jax.random.uniform(jax.random.fold_in(jax.random.fold_in(stream_key, 6), axis_at), (parts,), jnp.float32, smallest / len(split), top_value / len(split))
        gain = gain * jnp.repeat(jnp.exp(steps), dims[axis_at] // parts).reshape((-1,) + (1,) * (len(dims) - 1 - axis_at))
    return gain


def routed_block(rng, own, number, rows, amount, top, bound, slope):
    ranking = jax.random.permutation(rng, amount)
    heavy_load, common = load_shares(amount, rows * top, bound, slope, True), load_shares(amount, rows * top, bound, slope, False)
    places = jnp.arange(amount)

    def named(lengths, rotation):
        used = int((lengths > 0).sum())
        fixed = max(1, used // 4)
        shifted = fixed + (places - fixed + rotation * (used - fixed)) % max(1, amount - fixed)
        return jnp.zeros((amount,), jnp.int32).at[ranking[jnp.where(places < fixed, places, shifted)]].set(jnp.asarray(lengths, jnp.int32))

    lengths = jnp.where(number % 4 == 0, named(heavy_load, number // 4), named(common, number - number // 4 - 1))
    mixed = jax.random.permutation(jax.random.fold_in(own, 3), amount)
    giver, sink = mixed[0:amount // 2 * 2:2], mixed[1:amount // 2 * 2:2]
    slack = jnp.minimum(lengths[giver] - 1, bound - lengths[sink]) // 2
    slack = jnp.where((giver == ranking[0]) | (sink == ranking[0]) | (lengths[sink] == 0), 0, jnp.maximum(slack, 0))
    shifted = jax.random.randint(jax.random.fold_in(own, 4), (amount // 2,), 0, 1 << 20) % (slack + 1)
    lengths = lengths.at[giver].add(-shifted).at[sink].add(shifted)
    members = jnp.searchsorted(jnp.cumsum(lengths), jnp.arange(rows * top), side="right").astype(jnp.int32)
    listing = members.reshape(top, rows).T
    listing = listing[jax.random.permutation(jax.random.fold_in(own, 1), rows)]
    rotation = jax.random.randint(jax.random.fold_in(own, 2), (rows, 1), 0, top)
    return jnp.take_along_axis(listing, (jnp.arange(top)[None, :] + rotation) % top, axis=1)


def load_shares(count, total, limit, lean, full):
    weights = [(1 << 20) // math.isqrt(standing ** lean) + 1 for standing in range(1, count + 1)]
    largest = limit if full else min(limit, max(-(-total // count), total * weights[0] // sum(weights)))
    least = 1 if total - largest >= count - 1 else 0
    given, rest = [largest] + [least] * (count - 1), total - largest - least * (count - 1)
    while rest > 0:
        free = [i for i in range(1, count) if given[i] < largest] or [i for i in range(1, count) if given[i] < limit]
        mass, left = sum([weights[i] for i in free]), rest
        for i in free:
            more = min(limit - given[i], max(1, left * weights[i] // mass), rest)
            given[i] = given[i] + more
            rest = rest - more
    return np.array(given)


def normal_values(own_key, dims, deviation, reach, shards=(), kind=jnp.bfloat16):
    gain = block_scale(own_key, dims, shards, -0.22, 0.18) if shards else 1.0
    entries = jax.random.normal(own_key, dims, jnp.float32) * deviation * gain
    return jnp.minimum(jnp.maximum(entries, -reach), reach).astype(kind)


def setup_inputs(seed: int = 0) -> dict:
    splits = jax.random.split(jax.random.key(seed), 11)
    trial_factor = normal_values(splits[0], (K, NBF, NOCC), 1.0, 6.0, ((1, 128),))
    occupied = normal_values(splits[1], (NBF, NOCC), NOCC ** -0.5, 0.25, ((0, 128),))
    centers = jnp.clip(1.0 * jax.random.uniform(splits[2], (3, NBF), jnp.float32) ** block_scale(splits[2], (3, NBF), ((1, 128),), -0.2, 0.2), 0.0, 1.0)
    exponents = jnp.clip(jnp.exp(math.log(4.0) - 2.0794415 * jax.random.uniform(splits[3], (NBF,), jnp.float32) ** block_scale(splits[3], (NBF,), ((0, 128),), -0.2, 0.2)), 0.5, 4.0)
    wave_vectors = normal_values(splits[4], (3, NBF), 6.0, 36.0, ((1, 128),), jnp.float32)
    phases = jnp.clip(jax.random.uniform(splits[5], (NBF,), jnp.float32, -3.140625, 3.140625), -3.140625, 3.140625)
    points = jnp.clip(1.0 * jax.random.uniform(splits[6], (BATCHES, 3, GB), jnp.float32) ** block_scale(splits[6], (BATCHES, 3, GB), ((0, 128),), -0.2, 0.2), 0.0, 1.0)
    density = jnp.clip(jnp.exp(math.log(1.0) - 2.9957323 * jax.random.uniform(splits[7], (BATCHES, GB), jnp.float32) ** block_scale(splits[7], (BATCHES, GB), ((0, 128),), -0.2, 0.2)), 0.05, 1.0)
    weights = jnp.clip(jnp.exp(math.log(0.001) - 2.3025852 * jax.random.uniform(splits[8], (BATCHES, GB), jnp.float32) ** block_scale(splits[8], (BATCHES, GB), ((0, 128),), -0.2, 0.2)), 0.0001, 0.001)
    sources_keys = jax.random.split(jax.random.fold_in(splits[9], 1), BATCHES * NPAIR // (BATCH_DEV * NPAIR))
    sources_turns = jax.random.permutation(jax.random.fold_in(splits[9], 3), BATCHES * NPAIR // (BATCH_DEV * NPAIR))
    sources = jax.vmap(lambda own, number: routed_block(jax.random.fold_in(splits[9], 2), own, number, BATCH_DEV * NPAIR, COLS, 1, CAP, 2))(sources_keys, sources_turns).reshape((BATCHES, NPAIR, 1))
    return dict(trial_factor=trial_factor, occupied=occupied, centers=centers, exponents=exponents, wave_vectors=wave_vectors, phases=phases, points=points, density=density, weights=weights, sources=sources)


EXCHANGE_COEF = 0.75 * (3.0 / 3.141592653589793) ** (1.0 / 3.0)


def collocate(grid_points, func_centers, func_exponents, func_waves, func_phases):
    npoints = grid_points.shape[1]
    nfuncs = func_centers.shape[1]
    radius = jnp.zeros((npoints, nfuncs), jnp.float32)
    phase_sum = jnp.zeros((npoints, nfuncs), jnp.float32) + func_phases[None, :]
    for coordinate in range(3):
        offset = grid_points[coordinate][:, None] - func_centers[coordinate][None, :]
        radius = radius + offset * offset
        phase_sum = phase_sum + grid_points[coordinate][:, None] * func_waves[coordinate][None, :]
    return (jnp.exp(-func_exponents[None, :] * radius) * jnp.cos(phase_sum)).astype(jnp.bfloat16)


def batch_response(ground, quad_weights, row_values, col_values, pair_tiles):
    npoints = col_values.shape[0]
    row_tiles = pair_tiles.shape[0]
    col_span = pair_tiles.shape[1]
    tile_width = pair_tiles.shape[2]
    tile_size = row_values.shape[1] // row_tiles
    vectors = tile_width // tile_size
    col_phi = col_values.reshape(npoints, row_tiles, col_span).astype(jnp.float32)
    half_contracted = jnp.einsum('gax,axy->gay', col_phi, pair_tiles.astype(jnp.float32), precision=lax.Precision.HIGHEST)
    half_contracted = half_contracted.reshape(npoints, row_tiles, vectors, tile_size)
    row_phi = row_values.astype(jnp.float32).reshape(npoints, row_tiles, 1, tile_size)
    response_density = jnp.sum(half_contracted * row_phi, axis=(1, 3))
    kernel = -(4.0 / 9.0) * EXCHANGE_COEF * jnp.exp(-(2.0 / 3.0) * jnp.log(ground))
    potential = (quad_weights * kernel)[:, None] * response_density
    scaled = (potential[:, None, :, None] * row_phi).astype(jnp.bfloat16).reshape(npoints, row_tiles, tile_width)
    matrix = jnp.einsum('gax,gay->axy', col_phi, scaled.astype(jnp.float32), precision=lax.Precision.HIGHEST)
    return matrix.astype(jnp.bfloat16)


def reference(trial_factor, occupied, centers, exponents, wave_vectors, phases, points, density, weights, sources):
    span_row = TR * TB
    orbital_count = occupied.shape[1]
    tile_offsets = jnp.arange(TB, dtype=jnp.int32)
    pair_slots = jnp.arange(NPAIR, dtype=jnp.int32)

    def one_batch(position, response):
        position = jnp.asarray(position).astype(jnp.int32)
        row_block = (position // BATCH_DEV) // N_COL
        row_start = (row_block * span_row).astype(jnp.int32)
        row_factor = lax.dynamic_slice_in_dim(trial_factor, row_start, span_row, 1)
        column_tile = sources[position, :, 0] * TC + pair_slots % TC
        column_index = (column_tile[:, None] * TB + tile_offsets[None, :]).reshape(NPAIR * TB).astype(jnp.int32)
        factor_rows = jnp.take(occupied, column_index, axis=0).reshape(TR, TC, TB, orbital_count)
        pair_tiles = jnp.einsum('kami,abni->abnkm', row_factor.astype(jnp.float32).reshape(K, TR, TB, orbital_count), factor_rows.astype(jnp.float32), precision=lax.Precision.HIGHEST)
        pair_tiles = pair_tiles.astype(jnp.bfloat16).reshape(TR, TC * TB, K * TB)
        grid_points = points[position]
        row_values = collocate(grid_points, lax.dynamic_slice_in_dim(centers, row_start, span_row, 1), lax.dynamic_slice_in_dim(exponents, row_start, span_row, 0), lax.dynamic_slice_in_dim(wave_vectors, row_start, span_row, 1), lax.dynamic_slice_in_dim(phases, row_start, span_row, 0))
        col_values = collocate(grid_points, jnp.take(centers, column_index, axis=1), jnp.take(exponents, column_index), jnp.take(wave_vectors, column_index, axis=1), jnp.take(phases, column_index))
        pair_potential = batch_response(density[position], weights[position], row_values, col_values, pair_tiles)
        contrib = jnp.einsum('axkm,axi->amki', pair_potential.astype(jnp.float32).reshape(TR, TC * TB, K, TB), factor_rows.reshape(TR, TC * TB, orbital_count).astype(jnp.float32), precision=lax.Precision.HIGHEST)
        current = lax.dynamic_slice_in_dim(response, row_start, span_row, 0)
        return lax.dynamic_update_slice_in_dim(response, current + contrib.reshape(span_row, K, orbital_count), row_start, 0)

    start_value = jnp.zeros((NBF, K, orbital_count), jnp.float32)
    return lax.fori_loop(0, BATCHES, one_batch, start_value)
```

```python
import functools
import math

import jax
import jax.numpy as jnp
from jax import lax
from jax.experimental import pallas as pl
from jax.experimental.pallas import tpu as pltpu
from jax.sharding import PartitionSpec as P

BF = jnp.bfloat16
F32 = jnp.float32
MESH = pl.DeviceIdType.MESH
FULL = slice(None)
EXCHANGE_COEF = 0.75 * (3.0 / 3.141592653589793) ** (1.0 / 3.0)
S0, S1, S2, S3 = 6.283164044302474, -41.33714237110029, 81.34076888766828, -70.99343327209985
D0, D1, D2 = S0 / S3, S1 / S3, S2 / S3
LOG_S = math.log2(-S3)
LOG2E = math.log2(math.e)
TURN = 1.0 / (2.0 * math.pi)
GRID = 1024
CHUNK = 256


class Net:
    def __init__(self, send_sem, recv_sem):
        self.row, self.col = lax.axis_index("row"), lax.axis_index("col")
        self.pos = {"x": self.col // 4, "y": self.col % 4, "z": self.row // 2}
        self.core = self.row % 2
        self.send_sem, self.recv_sem = send_sem, recv_sem
        self.count = 0
        self.sent = []

    def at(self, dim, step):
        return lax.rem(self.pos[dim] + (step + 4), 4)

    def chip(self, dim, step):
        p = dict(self.pos)
        p[dim] = self.at(dim, step)
        return (p["z"] * 2 + self.core, p["x"] * 4 + p["y"])

    def partner(self):
        return (self.row + 1 - 2 * self.core, self.col)

    def copy(self, i, src, dst, device):
        return pltpu.make_async_remote_copy(
            src_ref=src,
            dst_ref=dst,
            send_sem=self.send_sem.at[i],
            recv_sem=self.recv_sem.at[i],
            device_id=device,
            device_id_type=MESH,
        )

    def send(self, src, dst, device):
        i = self.count
        self.count += 1
        c = self.copy(i, src, dst, device)
        c.start()
        self.sent.append(c)
        return i

    def arrived(self, i, dst):
        self.copy(i, dst, dst, self.partner()).wait_recv()

    def drain(self):
        for c in self.sent:
            c.wait_send()
        self.sent = []


def barrier(net):
    sem = pltpu.get_barrier_semaphore()
    peers = [net.partner()] + [net.chip(d, s) for d in "xyz" for s in (1, -1, 2)]
    for p in peers:
        pl.semaphore_signal(sem, inc=1, device_id=p, device_id_type=MESH)
    pl.semaphore_wait(sem, len(peers))


class Gather:
    def __init__(self, net, view, order, direct, forward=1):
        self.net, self.view, self.order, self.direct, self.forward = net, view, order, direct, forward
        self.phase = 0
        self.shared = []

    def index(self, **over):
        idx = dict(self.net.pos)
        for d in self.order[: self.phase]:
            idx[d] = FULL
        idx.update(over)
        return idx

    def start(self):
        net, d = self.net, self.order[self.phase]
        mine = self.view(self.index(), net.core)
        self.ids = {}
        for s in (1, -1) + ((2,) if self.direct[self.phase] else ()):
            self.ids[-s if s != 2 else 2] = net.send(mine, mine, net.chip(d, s))

    def take(self, s):
        net, d = self.net, self.order[self.phase]
        b = self.view(self.index(**{d: net.at(d, s)}), net.core)
        net.arrived(self.ids[s], b)
        if not self.direct[self.phase] and s == -self.forward:
            self.ids[2] = net.send(b, b, net.chip(d, self.forward))

    def step(self):
        for s in (-self.forward, self.forward, 2):
            self.take(s)
        self.phase += 1
        if self.phase < len(self.order):
            self.start()

    def share(self, s=None):
        d = self.order[self.phase]
        idx = self.index() if s is None else self.index(**{d: self.net.at(d, s)})
        b = self.view(idx, self.net.core)
        self.shared.append((self.net.send(b, b, self.net.partner()), idx))

    def get_shared(self):
        for i, idx in self.shared:
            self.net.arrived(i, self.view(idx, 1 - self.net.core))


def dot(a, b, ca=1, cb=0):
    return lax.dot_general(a, b, (((ca,), (cb,)), ((), ())), preferred_element_type=F32)


def splits(x):
    hi = x.astype(BF)
    rest = x - hi.astype(F32)
    mid = rest.astype(BF)
    return hi, mid, (rest - mid.astype(F32)).astype(BF)


def func_features(g):
    row = lax.broadcasted_iota(jnp.int32, g.shape, 0)
    ph = jnp.where((row >= 3) & (row != 6), g * TURN, 0.0)
    ex = g[6:7] * LOG2E
    c2 = g[0:1] * g[0:1] + g[1:2] * g[1:2] + g[2:3] * g[2:3]
    ee = jnp.where(row < 3, 2.0 * ex * g, jnp.where(row == 6, -ex, jnp.where(row == 7, LOG_S - ex * c2, 0.0)))
    hi, mid, lo = splits(jnp.concatenate([ph, ee], axis=0))
    return jnp.concatenate([hi, hi, hi, mid, mid, mid, lo, lo], axis=0)


def point_features(p):
    p0, p1, p2 = p[0:1], p[1:2], p[2:3]
    row = lax.broadcasted_iota(jnp.int32, (8, p.shape[1]), 0)
    rows = lambda *pairs: functools.reduce(lambda acc, rv: jnp.where(row == rv[0], rv[1], acc), pairs, jnp.zeros(row.shape, F32))
    ph = rows((3, p0), (4, p1), (5, p2), (7, 1.0))
    ee = rows((0, p0), (1, p1), (2, p2), (6, p0 * p0 + p1 * p1 + p2 * p2), (7, 1.0))
    zero = jnp.zeros_like(ph)
    out = []
    for parts in ([ph, zero], [zero, ee]):
        hi, mid, lo = splits(jnp.concatenate(parts, axis=0))
        out.append(jnp.concatenate([hi, mid, lo, hi, mid, lo, hi, mid], axis=0))
    return out


def basis(phase, exponent):
    r = phase - lax.round(phase, lax.RoundingMethod.TO_NEAREST_EVEN)
    z = jnp.abs(r) - 0.25
    y = z * z
    return (jnp.exp2(exponent) * (z * (((y + D2) * y + D1) * y + D0))).astype(BF)


def chunks():
    return [pl.ds(c, CHUNK) for c in range(0, GRID, CHUNK)]


def fused(
    occ, tri, cen, wav, exo, pha, pts, den, wts, src, out,
    O, T, G, par, FT, FR, PT, PP, phiR, phiC, B, rho, vk, Rb, H, A, S, A2,
    send_sem, recv_sem, local_sem,
):
    net = Net(send_sem, recv_sem)
    x, y, z, core = net.pos["x"], net.pos["y"], net.pos["z"], net.core
    local = [
        pltpu.make_async_copy(occ, O.at[x, y, z, core], local_sem.at[0]),
        pltpu.make_async_copy(tri, T.at[:, x, y], local_sem.at[1]),
    ]
    for c in local:
        c.start()
    par[...] = jnp.zeros_like(par)
    par[0:3, 0:64] = cen[...]
    par[3:6, 0:64] = wav[...]
    par[6:7, 0:64] = exo[...]
    par[7:8, 0:64] = pha[...]
    G[z, core, x, y] = par[...]
    barrier(net)
    for c in local:
        c.wait()

    gp = Gather(net, lambda i, c: G.at[i["z"], c, i["x"], i["y"]], "xyz", (1, 1, 1))
    go = [
        Gather(net, lambda i, c, p=p: O.at[i["x"], i["y"], i["z"], c, p], o, (1, 1, 0), f)
        for p, (o, f) in enumerate((("xyz", 1), ("yxz", -1), ("zxy", -1), ("zyx", -1)))
    ]
    gt = [Gather(net, lambda i, c, k=k: T.at[k, i["x"], i["y"]], o, (1, 0), -1) for k, o in enumerate(("xy", "yx"))]
    gp.start()
    for g in go + gt:
        g.start()

    for b in range(2):
        f = point_features(pts[b])
        for i in range(2):
            PT[b, i] = f[i]
            PP[b, i] = f[i].T
    gp.step()
    for g in gt + go:
        g.step()
    gp.step()
    gp.share()

    def tile_features(zz, cc, xx):
        return func_features(jnp.concatenate([G[zz, cc, xx, i][:, :64] for i in range(4)], axis=1))

    for a in range(4):
        FR[a] = tile_features(z, core, a).T

    def rows(lo, hi):
        def body(i, _):
            b, a = i // 4, i % 4
            for sl in chunks():
                phiR[b, a, :, sl] = basis(dot(FR[a], PT[b, 0, :, sl]), dot(FR[a], PT[b, 1, :, sl]))
            return 0

        lax.fori_loop(lo, hi, body, 0)

    def cols(lo, hi):
        def body(i, _):
            b, j = i // 8, i % 8
            f = FT[src[b, j, 0] * 2 + j % 2]
            for sl in chunks():
                phiC[b, j, sl, :] = basis(dot(PP[b, 0, sl], f), dot(PP[b, 1, sl], f))
            return 0

        lax.fori_loop(lo, hi, body, 0)

    rows(0, 2)
    for g in go:
        g.step()
        g.share()
    rows(2, 5)
    for s in (1, -1, 2):
        gp.take(s)
        gp.share(s)
    rows(5, 8)
    for g in gt:
        g.take(-g.forward)
    for g in go:
        g.take(-g.forward)
        g.share(-g.forward)
    gp.get_shared()

    def all_features(t, _):
        FT[t] = tile_features(t // 8, (t // 4) % 2, t % 4)
        return 0

    lax.fori_loop(0, 32, all_features, 0)
    cols(0, 5)
    for g in go:
        g.take(g.forward)
        g.share(g.forward)
    cols(5, 10)
    for g in gt:
        g.take(g.forward)
        g.take(2)
    cols(10, 16)
    for g in go:
        g.take(2)
        g.share(2)
    for g in go:
        g.get_shared()

    def half(i, _):
        b, a = i // 4, i % 4
        o = []
        for j in range(2):
            s = src[b, 2 * a + j, 0]
            o.append(O[s // 4, s % 4, 2 * j : 2 * j + 2].reshape(256, 512))
        for sl in chunks():
            B[i, sl, :] = (dot(phiC[b, 2 * a, sl, :], o[0]) + dot(phiC[b, 2 * a + 1, sl, :], o[1])).astype(BF)
        return 0

    lax.fori_loop(0, 8, half, 0)

    rho[...] = jnp.zeros_like(rho)

    def densities(i, _):
        b, a = i // 4, i % 4
        for sl in chunks():
            bb = B[i, sl, :]
            phi = phiR[b, a, :, sl].astype(F32)
            for k in range(2):
                cc = dot(T[k, a].reshape(256, 512), bb, 1, 1)
                rho[b, k : k + 1, sl] += jnp.sum(cc * phi, axis=0, keepdims=True)
        return 0

    lax.fori_loop(0, 8, densities, 0)
    for b in range(2):
        f = wts[b : b + 1, :] * (-(4.0 / 9.0) * EXCHANGE_COEF * jnp.exp(-(2.0 / 3.0) * jnp.log(den[b : b + 1, :])))
        for k in range(2):
            vk[b, k : k + 1, :] = f * rho[b, k : k + 1, :]

    def tile(k, a):
        acc = None
        for b in range(2):
            sc = (phiR[b, a].astype(F32) * vk[b, k : k + 1, :]).astype(BF)
            d = dot(sc, B[b * 4 + a])
            acc = d if acc is None else acc + d
        Rb[k, a] = acc.astype(BF).reshape(4, 64, 512)

    dims = ("x", "y")

    def chunk(k, c, half=FULL):
        return Rb.at[0, c, half] if k == 0 else Rb.at[1, half, c]

    lows, highs = pl.ds(0, 2), pl.ds(2, 2)
    ids = [{}, {}]

    def opposite(k):
        d = dims[k]
        c = net.at(d, 2)
        ids[k]["h0"] = net.send(chunk(k, c, lows), H.at[k, 0], net.chip(d, 1))
        ids[k]["h1"] = net.send(chunk(k, c, highs), H.at[k, 1], net.chip(d, -1))

    def neighbours(k):
        d = dims[k]
        for n, (s, hs) in enumerate(((1, lows), (-1, highs))):
            c = net.at(d, s)
            net.arrived(ids[k][f"h{n}"], H.at[k, n])
            part = chunk(k, c, hs)
            part[...] = (part[...].astype(F32) + H[k, n].astype(F32)).astype(BF)
            ids[k][f"a{n}"] = net.send(chunk(k, c), A.at[k, n], net.chip(d, s))

    def second(k):
        d, e = dims[k], dims[1 - k]
        for n in range(2):
            net.arrived(ids[k][f"a{n}"], A.at[k, n])
        total = chunk(k, net.pos[d])[...].astype(F32) + A[k, 0].astype(F32) + A[k, 1].astype(F32)
        S[k] = total.astype(BF)
        for n, s in enumerate((2, 1, -1)):
            ids[k][f"s{n}"] = net.send(S.at[k, net.at(e, s)], A2.at[k, n], net.chip(e, s))

    def finish(k):
        total = S[k, net.pos[dims[1 - k]]].astype(F32)
        for n in range(3):
            net.arrived(ids[k][f"s{n}"], A2.at[k, n])
            total = total + A2[k, n].astype(F32)
        out[:, k, :] = total

    def tiles_1(a, _):
        tile(1, a)
        return 0

    lax.fori_loop(0, 4, tiles_1, 0)
    opposite(1)
    tile(0, net.at("x", 2))
    opposite(0)
    tile(0, net.at("x", 1))
    tile(0, net.at("x", -1))
    neighbours(1)
    neighbours(0)
    tile(0, net.pos["x"])
    second(1)
    second(0)
    finish(1)
    finish(0)
    net.drain()


SEMS = 140


def per_device(tri, occ, cen, exo, wav, pha, pts, den, wts, src):
    vmem, hbm = pl.BlockSpec(memory_space=pltpu.VMEM), pl.BlockSpec(memory_space=pl.ANY)
    return pl.pallas_call(
        fused,
        out_shape=jax.ShapeDtypeStruct((64, 2, 512), F32),
        in_specs=[hbm, hbm] + [vmem] * 7 + [pl.BlockSpec(memory_space=pltpu.SMEM)],
        out_specs=vmem,
        scratch_shapes=[
            pltpu.VMEM((4, 4, 4, 2, 4, 16, 512), BF),
            pltpu.VMEM((2, 4, 4, 64, 512), BF),
            pltpu.VMEM((4, 2, 4, 4, 8, 128), F32),
            pltpu.VMEM((8, 128), F32),
            pltpu.VMEM((32, 128, 256), BF),
            pltpu.VMEM((4, 256, 128), BF),
            pltpu.VMEM((2, 2, 128, GRID), BF),
            pltpu.VMEM((2, 2, GRID, 128), BF),
            pltpu.VMEM((2, 4, 256, GRID), BF),
            pltpu.VMEM((2, 8, GRID, 256), BF),
            pltpu.VMEM((8, GRID, 512), BF),
            pltpu.VMEM((2, 2, GRID), F32),
            pltpu.VMEM((2, 2, GRID), F32),
            pltpu.VMEM((2, 4, 4, 64, 512), BF),
            pltpu.VMEM((2, 2, 2, 64, 512), BF),
            pltpu.VMEM((2, 2, 4, 64, 512), BF),
            pltpu.VMEM((2, 4, 64, 512), BF),
            pltpu.VMEM((2, 3, 64, 512), BF),
            pltpu.SemaphoreType.DMA((SEMS,)),
            pltpu.SemaphoreType.DMA((SEMS,)),
            pltpu.SemaphoreType.DMA((2,)),
        ],
        compiler_params=pltpu.CompilerParams(collective_id=0, has_side_effects=True, vmem_limit_bytes=62 * 2**20),
        name="fused",
    )(occ.reshape(4, 16, 512), tri, cen, wav, exo.reshape(1, 64), pha.reshape(1, 64), pts, den, wts, src)


def solution(mesh):
    both = ("row", "col")
    in_specs = (
        P(None, both, None),
        P(("col", "row"), None),
        P(None, both),
        P(both),
        P(None, both),
        P(both),
        P(both, None, None),
        P(both, None),
        P(both, None),
        P(both, None, None),
    )
    return jax.shard_map(per_device, mesh=mesh, in_specs=in_specs, out_specs=P(both, None, None), check_vma=False)
```

```python
import functools
import math

import jax
import jax.numpy as jnp
from jax import lax
from jax.experimental import pallas as pl
from jax.experimental.pallas import tpu as pltpu
from jax.sharding import PartitionSpec as P

BF = jnp.bfloat16
F32 = jnp.float32
MESH = pl.DeviceIdType.MESH
FULL = slice(None)
EXCHANGE_COEF = 0.75 * (3.0 / 3.141592653589793) ** (1.0 / 3.0)
S0, S1, S2, S3 = 6.283164044302474, -41.33714237110029, 81.34076888766828, -70.99343327209985
D0, D1, D2 = S0 / S3, S1 / S3, S2 / S3
LOG_S = math.log2(-S3)
LOG2E = math.log2(math.e)
TURN = 1.0 / (2.0 * math.pi)
GRID = 1024
CHUNK = 256


class Net:
    def __init__(self, send_sem, recv_sem):
        self.row, self.col = lax.axis_index("row"), lax.axis_index("col")
        self.pos = {"x": self.col // 4, "y": self.col % 4, "z": self.row // 2}
        self.core = self.row % 2
        self.send_sem, self.recv_sem = send_sem, recv_sem
        self.count = 0
        self.sent = []

    def at(self, dim, step):
        return lax.rem(self.pos[dim] + (step + 4), 4)

    def chip(self, dim, step):
        p = dict(self.pos)
        p[dim] = self.at(dim, step)
        return (p["z"] * 2 + self.core, p["x"] * 4 + p["y"])

    def partner(self):
        return (self.row + 1 - 2 * self.core, self.col)

    def copy(self, i, src, dst, device):
        return pltpu.make_async_remote_copy(
            src_ref=src,
            dst_ref=dst,
            send_sem=self.send_sem.at[i],
            recv_sem=self.recv_sem.at[i],
            device_id=device,
            device_id_type=MESH,
        )

    def send(self, src, dst, device):
        i = self.count
        self.count += 1
        c = self.copy(i, src, dst, device)
        c.start()
        self.sent.append(c)
        return i

    def arrived(self, i, dst):
        self.copy(i, dst, dst, self.partner()).wait_recv()

    def drain(self):
        for c in self.sent:
            c.wait_send()
        self.sent = []


def barrier(net):
    sem = pltpu.get_barrier_semaphore()
    peers = [net.partner()] + [net.chip(d, s) for d in "xyz" for s in (1, -1, 2)]
    for p in peers:
        pl.semaphore_signal(sem, inc=1, device_id=p, device_id_type=MESH)
    pl.semaphore_wait(sem, len(peers))


class Gather:
    def __init__(self, net, view, order, direct, forward=1):
        self.net, self.view, self.order, self.direct, self.forward = net, view, order, direct, forward
        self.phase = 0
        self.shared = []

    def index(self, **over):
        idx = dict(self.net.pos)
        for d in self.order[: self.phase]:
            idx[d] = FULL
        idx.update(over)
        return idx

    def start(self):
        net, d = self.net, self.order[self.phase]
        mine = self.view(self.index(), net.core)
        self.ids = {}
        for s in (1, -1) + ((2,) if self.direct[self.phase] else ()):
            self.ids[-s if s != 2 else 2] = net.send(mine, mine, net.chip(d, s))

    def take(self, s):
        net, d = self.net, self.order[self.phase]
        b = self.view(self.index(**{d: net.at(d, s)}), net.core)
        net.arrived(self.ids[s], b)
        if not self.direct[self.phase] and s == -self.forward:
            self.ids[2] = net.send(b, b, net.chip(d, self.forward))

    def step(self):
        for s in (-self.forward, self.forward, 2):
            self.take(s)
        self.phase += 1
        if self.phase < len(self.order):
            self.start()

    def share(self, s=None):
        d = self.order[self.phase]
        idx = self.index() if s is None else self.index(**{d: self.net.at(d, s)})
        b = self.view(idx, self.net.core)
        self.shared.append((self.net.send(b, b, self.net.partner()), idx))

    def get_shared(self):
        for i, idx in self.shared:
            self.net.arrived(i, self.view(idx, 1 - self.net.core))


def dot(a, b, ca=1, cb=0):
    return lax.dot_general(a, b, (((ca,), (cb,)), ((), ())), preferred_element_type=F32)


def splits(x):
    hi = x.astype(BF)
    rest = x - hi.astype(F32)
    mid = rest.astype(BF)
    return hi, mid, (rest - mid.astype(F32)).astype(BF)


def func_features(g):
    row = lax.broadcasted_iota(jnp.int32, g.shape, 0)
    ph = jnp.where((row >= 3) & (row != 6), g * TURN, 0.0)
    ex = g[6:7] * LOG2E
    c2 = g[0:1] * g[0:1] + g[1:2] * g[1:2] + g[2:3] * g[2:3]
    ee = jnp.where(row < 3, 2.0 * ex * g, jnp.where(row == 6, -ex, jnp.where(row == 7, LOG_S - ex * c2, 0.0)))
    hi, mid, lo = splits(jnp.concatenate([ph, ee], axis=0))
    return jnp.concatenate([hi, hi, hi, mid, mid, mid, lo, lo], axis=0)


def point_features(p):
    p0, p1, p2 = p
    row = lax.broadcasted_iota(jnp.int32, (8, p0.shape[1]), 0)
    rows = lambda *pairs: functools.reduce(lambda acc, rv: jnp.where(row == rv[0], rv[1], acc), pairs, jnp.zeros(row.shape, F32))
    ph = rows((3, p0), (4, p1), (5, p2), (7, 1.0))
    ee = rows((0, p0), (1, p1), (2, p2), (6, p0 * p0 + p1 * p1 + p2 * p2), (7, 1.0))
    zero = jnp.zeros_like(ph)
    out = []
    for parts in ([ph, zero], [zero, ee]):
        hi, mid, lo = splits(jnp.concatenate(parts, axis=0))
        out.append(jnp.concatenate([hi, mid, lo, hi, mid, lo, hi, mid], axis=0))
    return out


def basis(phase, exponent):
    r = phase - lax.round(phase, lax.RoundingMethod.TO_NEAREST_EVEN)
    z = jnp.abs(r) - 0.25
    y = z * z
    return (jnp.exp2(exponent) * (z * (((y + D2) * y + D1) * y + D0))).astype(BF)


def chunks():
    return [pl.ds(c, CHUNK) for c in range(0, GRID, CHUNK)]


def fused(
    occ, tri, cen, wav, exo, pha, pts, den, wts, src, out,
    O, T, G, par, FT, FR, PT, PP, phiR, phiC, B, rho, vk, Rb, H, A, S, A2,
    send_sem, recv_sem, local_sem,
):
    net = Net(send_sem, recv_sem)
    x, y, z, core = net.pos["x"], net.pos["y"], net.pos["z"], net.core
    local = [
        pltpu.make_async_copy(occ, O.at[x, y, z, core], local_sem.at[0]),
        pltpu.make_async_copy(tri, T.at[:, x, y], local_sem.at[1]),
    ]
    for c in local:
        c.start()
    par[...] = jnp.zeros_like(par)
    par[0:3, 0:64] = cen[...]
    par[3:6, 0:64] = wav[...]
    par[6:7, 0:64] = exo[...]
    par[7:8, 0:64] = pha[...]
    G[z, core, x, y] = par[...]
    barrier(net)
    for c in local:
        c.wait()

    gp = Gather(net, lambda i, c: G.at[i["z"], c, i["x"], i["y"]], "xyz", (1, 1, 1))
    go = [
        Gather(net, lambda i, c, p=p: O.at[i["x"], i["y"], i["z"], c, p], o, (1, 1, 0), f)
        for p, (o, f) in enumerate((("xyz", 1), ("yxz", -1), ("zxy", -1), ("zyx", -1)))
    ]
    gt = [Gather(net, lambda i, c, k=k: T.at[k, i["x"], i["y"]], o, (1, 0), -1) for k, o in enumerate(("xy", "yx"))]
    gp.start()
    for g in go + gt:
        g.start()

    for b in range(2):
        f = point_features([pts[i, b : b + 1, :] for i in range(3)])
        for i in range(2):
            PT[b, i] = f[i]
            PP[b, i] = f[i].T
    gp.step()
    for g in go + gt:
        g.step()
    gp.step()
    gp.share()

    def tile_features(zz, cc, xx):
        return func_features(jnp.concatenate([G[zz, cc, xx, i][:, :64] for i in range(4)], axis=1))

    for a in range(4):
        FR[a] = tile_features(z, core, a).T

    def rows(lo, hi):
        def body(i, _):
            b, a = i // 4, i % 4
            for sl in chunks():
                phiR[b, a, :, sl] = basis(dot(FR[a], PT[b, 0, :, sl]), dot(FR[a], PT[b, 1, :, sl]))
            return 0

        lax.fori_loop(lo, hi, body, 0)

    def cols(lo, hi):
        def body(i, _):
            b, j = i // 8, i % 8
            f = FT[src[b, 0, j] * 2 + j % 2]
            for sl in chunks():
                phiC[b, j, sl, :] = basis(dot(PP[b, 0, sl], f), dot(PP[b, 1, sl], f))
            return 0

        lax.fori_loop(lo, hi, body, 0)

    rows(0, 2)
    for g in go:
        g.step()
        g.share()
    rows(2, 5)
    for s in (1, -1, 2):
        gp.take(s)
        gp.share(s)
    rows(5, 8)
    for g in gt:
        g.take(-g.forward)
    for g in go:
        g.take(-g.forward)
        g.share(-g.forward)
    gp.get_shared()

    def all_features(t, _):
        FT[t] = tile_features(t // 8, (t // 4) % 2, t % 4)
        return 0

    lax.fori_loop(0, 32, all_features, 0)
    cols(0, 5)
    for g in go:
        g.take(g.forward)
        g.share(g.forward)
    cols(5, 10)
    for g in gt:
        g.take(g.forward)
        g.take(2)
    cols(10, 16)
    for g in go:
        g.take(2)
        g.share(2)
    for g in go:
        g.get_shared()

    def half(i, _):
        b, a = i // 4, i % 4
        o = []
        for j in range(2):
            s = src[b, 0, 2 * a + j]
            o.append(O[s // 4, s % 4, 2 * j : 2 * j + 2].reshape(256, 512))
        for sl in chunks():
            B[i, sl, :] = (dot(phiC[b, 2 * a, sl, :], o[0]) + dot(phiC[b, 2 * a + 1, sl, :], o[1])).astype(BF)
        return 0

    lax.fori_loop(0, 8, half, 0)

    rho[...] = jnp.zeros_like(rho)

    def densities(i, _):
        b, a = i // 4, i % 4
        for sl in chunks():
            bb = B[i, sl, :]
            phi = phiR[b, a, :, sl].astype(F32)
            for k in range(2):
                cc = dot(T[k, a].reshape(256, 512), bb, 1, 1)
                rho[b, k : k + 1, sl] += jnp.sum(cc * phi, axis=0, keepdims=True)
        return 0

    lax.fori_loop(0, 8, densities, 0)
    for b in range(2):
        f = wts[b : b + 1, :] * (-(4.0 / 9.0) * EXCHANGE_COEF * jnp.exp(-(2.0 / 3.0) * jnp.log(den[b : b + 1, :])))
        for k in range(2):
            vk[b, k : k + 1, :] = f * rho[b, k : k + 1, :]

    def tile(k, a):
        acc = None
        for b in range(2):
            sc = (phiR[b, a].astype(F32) * vk[b, k : k + 1, :]).astype(BF)
            d = dot(sc, B[b * 4 + a])
            acc = d if acc is None else acc + d
        Rb[k, a] = acc.astype(BF).reshape(4, 64, 512)

    dims = ("x", "y")

    def chunk(k, c, half=FULL):
        return Rb.at[0, c, half] if k == 0 else Rb.at[1, half, c]

    lows, highs = pl.ds(0, 2), pl.ds(2, 2)
    ids = [{}, {}]

    def opposite(k):
        d = dims[k]
        c = net.at(d, 2)
        ids[k]["h0"] = net.send(chunk(k, c, lows), H.at[k, 0], net.chip(d, 1))
        ids[k]["h1"] = net.send(chunk(k, c, highs), H.at[k, 1], net.chip(d, -1))

    def neighbours(k):
        d = dims[k]
        for n, (s, hs) in enumerate(((1, lows), (-1, highs))):
            c = net.at(d, s)
            net.arrived(ids[k][f"h{n}"], H.at[k, n])
            part = chunk(k, c, hs)
            part[...] = (part[...].astype(F32) + H[k, n].astype(F32)).astype(BF)
            ids[k][f"a{n}"] = net.send(chunk(k, c), A.at[k, n], net.chip(d, s))

    def second(k):
        d, e = dims[k], dims[1 - k]
        for n in range(2):
            net.arrived(ids[k][f"a{n}"], A.at[k, n])
        total = chunk(k, net.pos[d])[...].astype(F32) + A[k, 0].astype(F32) + A[k, 1].astype(F32)
        S[k] = total.astype(BF)
        for n, s in enumerate((2, 1, -1)):
            ids[k][f"s{n}"] = net.send(S.at[k, net.at(e, s)], A2.at[k, n], net.chip(e, s))

    def finish(k):
        total = S[k, net.pos[dims[1 - k]]].astype(F32)
        for n in range(3):
            net.arrived(ids[k][f"s{n}"], A2.at[k, n])
            total = total + A2[k, n].astype(F32)
        out[:, k, :] = total

    def tiles_1(a, _):
        tile(1, a)
        return 0

    lax.fori_loop(0, 4, tiles_1, 0)
    opposite(1)
    tile(0, net.at("x", 2))
    opposite(0)
    tile(0, net.at("x", 1))
    tile(0, net.at("x", -1))
    neighbours(1)
    neighbours(0)
    tile(0, net.pos["x"])
    second(1)
    second(0)
    finish(1)
    finish(0)
    net.drain()


SEMS = 140


def per_device(tri, occ, cen, exo, wav, pha, pts, den, wts, src):
    vmem, hbm = pl.BlockSpec(memory_space=pltpu.VMEM), pl.BlockSpec(memory_space=pl.ANY)
    return pl.pallas_call(
        fused,
        out_shape=jax.ShapeDtypeStruct((64, 2, 512), F32),
        in_specs=[hbm, hbm] + [vmem] * 7 + [pl.BlockSpec(memory_space=pltpu.SMEM)],
        out_specs=vmem,
        scratch_shapes=[
            pltpu.VMEM((4, 4, 4, 2, 4, 16, 512), BF),
            pltpu.VMEM((2, 4, 4, 64, 512), BF),
            pltpu.VMEM((4, 2, 4, 4, 8, 128), F32),
            pltpu.VMEM((8, 128), F32),
            pltpu.VMEM((32, 128, 256), BF),
            pltpu.VMEM((4, 256, 128), BF),
            pltpu.VMEM((2, 2, 128, GRID), BF),
            pltpu.VMEM((2, 2, GRID, 128), BF),
            pltpu.VMEM((2, 4, 256, GRID), BF),
            pltpu.VMEM((2, 8, GRID, 256), BF),
            pltpu.VMEM((8, GRID, 512), BF),
            pltpu.VMEM((2, 2, GRID), F32),
            pltpu.VMEM((2, 2, GRID), F32),
            pltpu.VMEM((2, 4, 4, 64, 512), BF),
            pltpu.VMEM((2, 2, 2, 64, 512), BF),
            pltpu.VMEM((2, 2, 4, 64, 512), BF),
            pltpu.VMEM((2, 4, 64, 512), BF),
            pltpu.VMEM((2, 3, 64, 512), BF),
            pltpu.SemaphoreType.DMA((SEMS,)),
            pltpu.SemaphoreType.DMA((SEMS,)),
            pltpu.SemaphoreType.DMA((2,)),
        ],
        compiler_params=pltpu.CompilerParams(collective_id=0, has_side_effects=True, vmem_limit_bytes=62 * 2**20),
        name="fused",
    )(occ.reshape(4, 16, 512), tri, cen, wav, exo.reshape(1, 64), pha.reshape(1, 64), pts.transpose(1, 0, 2), den, wts, src.transpose(0, 2, 1))


def solution(mesh):
    both = ("row", "col")
    in_specs = (
        P(None, both, None),
        P(("col", "row"), None),
        P(None, both),
        P(both),
        P(None, both),
        P(both),
        P(both, None, None),
        P(both, None),
        P(both, None),
        P(both, None, None),
    )
    return jax.shard_map(per_device, mesh=mesh, in_specs=in_specs, out_specs=P(both, None, None), check_vma=False)
```

```python
import functools
import math

import jax
import jax.numpy as jnp
from jax import lax
from jax.experimental import pallas as pl
from jax.experimental.pallas import tpu as pltpu
from jax.sharding import PartitionSpec as P

BF = jnp.bfloat16
F32 = jnp.float32
MESH = pl.DeviceIdType.MESH
FULL = slice(None)
EXCHANGE_COEF = 0.75 * (3.0 / 3.141592653589793) ** (1.0 / 3.0)
S0, S1, S2, S3 = 6.283164044302474, -41.33714237110029, 81.34076888766828, -70.99343327209985
D0, D1, D2 = S0 / S3, S1 / S3, S2 / S3
LOG_S = math.log2(-S3)
LOG2E = math.log2(math.e)
TURN = 1.0 / (2.0 * math.pi)
GRID = 1024
CHUNK = 256


class Net:
    def __init__(self, send_sem, recv_sem):
        self.row, self.col = lax.axis_index("row"), lax.axis_index("col")
        self.pos = {"x": self.col // 4, "y": self.col % 4, "z": self.row // 2}
        self.core = self.row % 2
        self.send_sem, self.recv_sem = send_sem, recv_sem
        self.count = 0
        self.sent = []

    def at(self, dim, step):
        return lax.rem(self.pos[dim] + (step + 4), 4)

    def chip(self, dim, step):
        p = dict(self.pos)
        p[dim] = self.at(dim, step)
        return (p["z"] * 2 + self.core, p["x"] * 4 + p["y"])

    def partner(self):
        return (self.row + 1 - 2 * self.core, self.col)

    def copy(self, i, src, dst, device):
        return pltpu.make_async_remote_copy(
            src_ref=src,
            dst_ref=dst,
            send_sem=self.send_sem.at[i],
            recv_sem=self.recv_sem.at[i],
            device_id=device,
            device_id_type=MESH,
        )

    def send(self, src, dst, device):
        i = self.count
        self.count += 1
        c = self.copy(i, src, dst, device)
        c.start()
        self.sent.append(c)
        return i

    def arrived(self, i, dst):
        self.copy(i, dst, dst, self.partner()).wait_recv()

    def drain(self):
        for c in self.sent:
            c.wait_send()
        self.sent = []


def barrier(net):
    sem = pltpu.get_barrier_semaphore()
    peers = [net.partner()] + [net.chip(d, s) for d in "xyz" for s in (1, -1, 2)]
    for p in peers:
        pl.semaphore_signal(sem, inc=1, device_id=p, device_id_type=MESH)
    pl.semaphore_wait(sem, len(peers))


class Gather:
    def __init__(self, net, view, order, direct, forward=1):
        self.net, self.view, self.order, self.direct, self.forward = net, view, order, direct, forward
        self.phase = 0
        self.shared = []

    def index(self, **over):
        idx = dict(self.net.pos)
        for d in self.order[: self.phase]:
            idx[d] = FULL
        idx.update(over)
        return idx

    def start(self):
        net, d = self.net, self.order[self.phase]
        mine = self.view(self.index(), net.core)
        self.ids = {}
        for s in (1, -1) + ((2,) if self.direct[self.phase] else ()):
            self.ids[-s if s != 2 else 2] = net.send(mine, mine, net.chip(d, s))

    def take(self, s):
        net, d = self.net, self.order[self.phase]
        b = self.view(self.index(**{d: net.at(d, s)}), net.core)
        net.arrived(self.ids[s], b)
        if not self.direct[self.phase] and s == -self.forward:
            self.ids[2] = net.send(b, b, net.chip(d, self.forward))

    def step(self):
        for s in (-self.forward, self.forward, 2):
            self.take(s)
        self.phase += 1
        if self.phase < len(self.order):
            self.start()

    def share(self, s=None):
        d = self.order[self.phase]
        idx = self.index() if s is None else self.index(**{d: self.net.at(d, s)})
        b = self.view(idx, self.net.core)
        self.shared.append((self.net.send(b, b, self.net.partner()), idx))

    def get_shared(self):
        for i, idx in self.shared:
            self.net.arrived(i, self.view(idx, 1 - self.net.core))


def dot(a, b, ca=1, cb=0):
    return lax.dot_general(a, b, (((ca,), (cb,)), ((), ())), preferred_element_type=F32)


def splits(x):
    hi = x.astype(BF)
    rest = x - hi.astype(F32)
    mid = rest.astype(BF)
    return hi, mid, (rest - mid.astype(F32)).astype(BF)


def func_features(g):
    row = lax.broadcasted_iota(jnp.int32, g.shape, 0)
    ph = jnp.where((row >= 3) & (row != 6), g * TURN, 0.0)
    ex = g[6:7] * LOG2E
    c2 = g[0:1] * g[0:1] + g[1:2] * g[1:2] + g[2:3] * g[2:3]
    ee = jnp.where(row < 3, 2.0 * ex * g, jnp.where(row == 6, -ex, jnp.where(row == 7, LOG_S - ex * c2, 0.0)))
    hi, mid, lo = splits(jnp.concatenate([ph, ee], axis=0))
    return jnp.concatenate([hi, hi, hi, mid, mid, mid, lo, lo], axis=0)


def point_features(p):
    p0, p1, p2 = p
    row = lax.broadcasted_iota(jnp.int32, (8, p0.shape[1]), 0)
    rows = lambda *pairs: functools.reduce(lambda acc, rv: jnp.where(row == rv[0], rv[1], acc), pairs, jnp.zeros(row.shape, F32))
    ph = rows((3, p0), (4, p1), (5, p2), (7, 1.0))
    ee = rows((0, p0), (1, p1), (2, p2), (6, p0 * p0 + p1 * p1 + p2 * p2), (7, 1.0))
    zero = jnp.zeros_like(ph)
    out = []
    for parts in ([ph, zero], [zero, ee]):
        hi, mid, lo = splits(jnp.concatenate(parts, axis=0))
        out.append(jnp.concatenate([hi, mid, lo, hi, mid, lo, hi, mid], axis=0))
    return out


def basis(phase, exponent):
    r = phase - lax.round(phase, lax.RoundingMethod.TO_NEAREST_EVEN)
    z = jnp.abs(r) - 0.25
    y = z * z
    return (jnp.exp2(exponent) * (z * (((y + D2) * y + D1) * y + D0))).astype(BF)


def chunks():
    return [pl.ds(c, CHUNK) for c in range(0, GRID, CHUNK)]


def fused(
    occ, tri, cen, wav, exo, pha, pts, den, wts, src, out,
    O, T, G, par, FT, FR, PT, PP, phiR, phiC, B, rho, vk, Rb, H, A, S, A2,
    send_sem, recv_sem, local_sem,
):
    net = Net(send_sem, recv_sem)
    x, y, z, core = net.pos["x"], net.pos["y"], net.pos["z"], net.core
    local = [
        pltpu.make_async_copy(occ, O.at[x, y, z, core], local_sem.at[0]),
        pltpu.make_async_copy(tri, T.at[:, x, y], local_sem.at[1]),
    ]
    for c in local:
        c.start()
    par[...] = jnp.zeros_like(par)
    par[0:3, 0:64] = cen[...]
    par[3:6, 0:64] = wav[...]
    par[6:7, 0:64] = exo[...]
    par[7:8, 0:64] = pha[...]
    G[z, core, x, y] = par[...]
    barrier(net)
    for c in local:
        c.wait()

    gp = Gather(net, lambda i, c: G.at[i["z"], c, i["x"], i["y"]], "xyz", (1, 1, 1))
    go = [
        Gather(net, lambda i, c, p=p: O.at[i["x"], i["y"], i["z"], c, p], o, (1, 1, 0), f)
        for p, (o, f) in enumerate((("xyz", 1), ("yxz", -1), ("zxy", -1), ("zyx", -1)))
    ]
    gt = [Gather(net, lambda i, c, k=k: T.at[k, i["x"], i["y"]], o, (1, 0), -1) for k, o in enumerate(("xy", "yx"))]
    gp.start()
    for g in go + gt:
        g.start()

    for b in range(2):
        f = point_features([pts[i, b : b + 1, :] for i in range(3)])
        for i in range(2):
            PT[b, i] = f[i]
            PP[b, i] = f[i].T
    gp.step()
    for g in go + gt:
        g.step()
    gp.step()
    gp.share()

    def tile_features(zz, cc, xx):
        return func_features(jnp.concatenate([G[zz, cc, xx, i][:, :64] for i in range(4)], axis=1))

    for a in range(4):
        FR[a] = tile_features(z, core, a).T

    def rows(lo, hi):
        def body(i, _):
            b, a = i // 4, i % 4
            for sl in chunks():
                phiR[b, a, :, sl] = basis(dot(FR[a], PT[b, 0, :, sl]), dot(FR[a], PT[b, 1, :, sl]))
            return 0

        lax.fori_loop(lo, hi, body, 0)

    def cols(lo, hi):
        def body(i, _):
            b, j = i // 8, i % 8
            f = FT[src[b, 0, j] * 2 + j % 2]
            for sl in chunks():
                phiC[b, j, sl, :] = basis(dot(PP[b, 0, sl], f), dot(PP[b, 1, sl], f))
            return 0

        lax.fori_loop(lo, hi, body, 0)

    rows(0, 2)
    for g in go:
        g.step()
        g.share()
    rows(2, 5)
    for s in (1, -1, 2):
        gp.take(s)
        gp.share(s)
    rows(5, 8)
    for g in go:
        g.take(-g.forward)
        g.share(-g.forward)
    for g in gt:
        g.take(-g.forward)
    gp.get_shared()

    def all_features(t, _):
        FT[t] = tile_features(t // 8, (t // 4) % 2, t % 4)
        return 0

    lax.fori_loop(0, 32, all_features, 0)
    cols(0, 5)
    for g in go:
        g.take(g.forward)
        g.share(g.forward)
    cols(5, 16)
    for g in go:
        g.take(2)
        g.share(2)
    for g in go:
        g.get_shared()

    def half(i, _):
        b, a = i // 4, i % 4
        o = []
        for j in range(2):
            s = src[b, 0, 2 * a + j]
            o.append(O[s // 4, s % 4, 2 * j : 2 * j + 2].reshape(256, 512))
        for sl in chunks():
            B[i, sl, :] = (dot(phiC[b, 2 * a, sl, :], o[0]) + dot(phiC[b, 2 * a + 1, sl, :], o[1])).astype(BF)
        return 0

    rho[...] = jnp.zeros_like(rho)

    def densities(i):
        b, a = i // 4, i % 4
        factors = jnp.concatenate([T[0, a].reshape(256, 512), T[1, a].reshape(256, 512)], axis=0)
        for sl in chunks():
            cc = dot(factors, B[i, sl, :], 1, 1)
            phi = phiR[b, a, :, sl].astype(F32)
            for k in range(2):
                part = cc[k * 256 : (k + 1) * 256] * phi
                rho[b, k : k + 1, sl] += jnp.sum(part, axis=0, keepdims=True)

    def both(i, _):
        densities(i - 4)
        half(i, 0)
        return 0

    def last(i, _):
        densities(i)
        return 0

    lax.fori_loop(0, 4, half, 0)
    for g in gt:
        g.take(g.forward)
        g.take(2)
    lax.fori_loop(4, 8, both, 0)
    lax.fori_loop(4, 8, last, 0)
    for b in range(2):
        f = wts[b : b + 1, :] * (-(4.0 / 9.0) * EXCHANGE_COEF * jnp.exp(-(2.0 / 3.0) * jnp.log(den[b : b + 1, :])))
        for k in range(2):
            vk[b, k : k + 1, :] = f * rho[b, k : k + 1, :]

    def tile(k, a):
        acc = None
        for b in range(2):
            sc = (phiR[b, a].astype(F32) * vk[b, k : k + 1, :]).astype(BF)
            d = dot(sc, B[b * 4 + a])
            acc = d if acc is None else acc + d
        Rb[k, a] = acc.astype(BF).reshape(4, 64, 512)

    dims = ("x", "y")

    def chunk(k, c, half=FULL):
        return Rb.at[0, c, half] if k == 0 else Rb.at[1, half, c]

    lows, highs = pl.ds(0, 2), pl.ds(2, 2)
    ids = [{}, {}]

    def opposite(k):
        d = dims[k]
        c = net.at(d, 2)
        ids[k]["h0"] = net.send(chunk(k, c, lows), H.at[k, 0], net.chip(d, 1))
        ids[k]["h1"] = net.send(chunk(k, c, highs), H.at[k, 1], net.chip(d, -1))

    def own_halves(k):
        d = dims[k]
        for n, (s, hs, part) in enumerate(((1, highs, 1), (-1, lows, 0))):
            ids[k][f"o{n}"] = net.send(chunk(k, net.at(d, s), hs), A.at[k, n, pl.ds(2 * part, 2)], net.chip(d, s))

    def summed_halves(k):
        d = dims[k]
        for n, (s, hs, part) in enumerate(((1, lows, 0), (-1, highs, 1))):
            net.arrived(ids[k][f"h{n}"], H.at[k, n])
            piece = chunk(k, net.at(d, s), hs)
            piece[...] = (piece[...].astype(F32) + H[k, n].astype(F32)).astype(BF)
            ids[k][f"a{n}"] = net.send(piece, A.at[k, n, pl.ds(2 * part, 2)], net.chip(d, s))

    def second(k):
        d, e = dims[k], dims[1 - k]
        for n, part in enumerate((0, 1)):
            net.arrived(ids[k][f"o{n}"], A.at[k, n, pl.ds(2 - 2 * part, 2)])
            net.arrived(ids[k][f"a{n}"], A.at[k, n, pl.ds(2 * part, 2)])
        total = chunk(k, net.pos[d])[...].astype(F32) + A[k, 0].astype(F32) + A[k, 1].astype(F32)
        S[k] = total.astype(BF)
        for n, s in enumerate((2, 1, -1)):
            ids[k][f"s{n}"] = net.send(S.at[k, net.at(e, s)], A2.at[k, n], net.chip(e, s))

    def finish(k):
        total = S[k, net.pos[dims[1 - k]]].astype(F32)
        for n in range(3):
            net.arrived(ids[k][f"s{n}"], A2.at[k, n])
            total = total + A2[k, n].astype(F32)
        out[:, k, :] = total

    def tiles_1(a, _):
        tile(1, a)
        return 0

    lax.fori_loop(0, 4, tiles_1, 0)
    opposite(1)
    own_halves(1)
    tile(0, net.at("x", 2))
    opposite(0)
    tile(0, net.at("x", 1))
    tile(0, net.at("x", -1))
    own_halves(0)
    summed_halves(1)
    summed_halves(0)
    tile(0, net.pos["x"])
    second(1)
    second(0)
    finish(1)
    finish(0)
    net.drain()


SEMS = 140


def per_device(tri, occ, cen, exo, wav, pha, pts, den, wts, src):
    vmem, hbm = pl.BlockSpec(memory_space=pltpu.VMEM), pl.BlockSpec(memory_space=pl.ANY)
    return pl.pallas_call(
        fused,
        out_shape=jax.ShapeDtypeStruct((64, 2, 512), F32),
        in_specs=[hbm, hbm] + [vmem] * 7 + [pl.BlockSpec(memory_space=pltpu.SMEM)],
        out_specs=vmem,
        scratch_shapes=[
            pltpu.VMEM((4, 4, 4, 2, 4, 16, 512), BF),
            pltpu.VMEM((2, 4, 4, 64, 512), BF),
            pltpu.VMEM((4, 2, 4, 4, 8, 128), F32),
            pltpu.VMEM((8, 128), F32),
            pltpu.VMEM((32, 128, 256), BF),
            pltpu.VMEM((4, 256, 128), BF),
            pltpu.VMEM((2, 2, 128, GRID), BF),
            pltpu.VMEM((2, 2, GRID, 128), BF),
            pltpu.VMEM((2, 4, 256, GRID), BF),
            pltpu.VMEM((2, 8, GRID, 256), BF),
            pltpu.VMEM((8, GRID, 512), BF),
            pltpu.VMEM((2, 2, GRID), F32),
            pltpu.VMEM((2, 2, GRID), F32),
            pltpu.VMEM((2, 4, 4, 64, 512), BF),
            pltpu.VMEM((2, 2, 2, 64, 512), BF),
            pltpu.VMEM((2, 2, 4, 64, 512), BF),
            pltpu.VMEM((2, 4, 64, 512), BF),
            pltpu.VMEM((2, 3, 64, 512), BF),
            pltpu.SemaphoreType.DMA((SEMS,)),
            pltpu.SemaphoreType.DMA((SEMS,)),
            pltpu.SemaphoreType.DMA((2,)),
        ],
        compiler_params=pltpu.CompilerParams(collective_id=0, has_side_effects=True, vmem_limit_bytes=62 * 2**20),
        name="fused",
    )(occ.reshape(4, 16, 512), tri, cen, wav, exo.reshape(1, 64), pha.reshape(1, 64), pts.transpose(1, 0, 2), den, wts, src.transpose(0, 2, 1))


def solution(mesh):
    both = ("row", "col")
    in_specs = (
        P(None, both, None),
        P(("col", "row"), None),
        P(None, both),
        P(both),
        P(None, both),
        P(both),
        P(both, None, None),
        P(both, None),
        P(both, None),
        P(both, None, None),
    )
    return jax.shard_map(per_device, mesh=mesh, in_specs=in_specs, out_specs=P(both, None, None), check_vma=False)
```

```python
import functools
import math

import jax
import jax.numpy as jnp
from jax import lax
from jax.experimental import pallas as pl
from jax.experimental.pallas import tpu as pltpu
from jax.sharding import PartitionSpec as P

BF = jnp.bfloat16
F32 = jnp.float32
MESH = pl.DeviceIdType.MESH
FULL = slice(None)
EXCHANGE_COEF = 0.75 * (3.0 / 3.141592653589793) ** (1.0 / 3.0)
S0, S1, S2, S3 = 6.283164044302474, -41.33714237110029, 81.34076888766828, -70.99343327209985
D0, D1, D2 = S0 / S3, S1 / S3, S2 / S3
LOG_S = math.log2(-S3)
LOG2E = math.log2(math.e)
TURN = 1.0 / (2.0 * math.pi)
GRID = 1024
CHUNK = 256


class Net:
    def __init__(self, send_sem, recv_sem):
        self.row, self.col = lax.axis_index("row"), lax.axis_index("col")
        self.pos = {"x": self.col // 4, "y": self.col % 4, "z": self.row // 2}
        self.core = self.row % 2
        self.send_sem, self.recv_sem = send_sem, recv_sem
        self.count = 0
        self.sent = []

    def at(self, dim, step):
        return lax.rem(self.pos[dim] + (step + 4), 4)

    def chip(self, dim, step):
        p = dict(self.pos)
        p[dim] = self.at(dim, step)
        return (p["z"] * 2 + self.core, p["x"] * 4 + p["y"])

    def partner(self):
        return (self.row + 1 - 2 * self.core, self.col)

    def copy(self, i, src, dst, device):
        return pltpu.make_async_remote_copy(
            src_ref=src,
            dst_ref=dst,
            send_sem=self.send_sem.at[i],
            recv_sem=self.recv_sem.at[i],
            device_id=device,
            device_id_type=MESH,
        )

    def send(self, src, dst, device):
        i = self.count
        self.count += 1
        c = self.copy(i, src, dst, device)
        c.start()
        self.sent.append(c)
        return i

    def arrived(self, i, dst):
        self.copy(i, dst, dst, self.partner()).wait_recv()

    def drain(self):
        for c in self.sent:
            c.wait_send()
        self.sent = []


def barrier(net):
    sem = pltpu.get_barrier_semaphore()
    peers = [net.partner()] + [net.chip(d, s) for d in "xyz" for s in (1, -1, 2)]
    for p in peers:
        pl.semaphore_signal(sem, inc=1, device_id=p, device_id_type=MESH)
    pl.semaphore_wait(sem, len(peers))


class Gather:
    def __init__(self, net, view, order, direct, forward=1):
        self.net, self.view, self.order, self.direct, self.forward = net, view, order, direct, forward
        self.phase = 0
        self.shared = []

    def index(self, **over):
        idx = dict(self.net.pos)
        for d in self.order[: self.phase]:
            idx[d] = FULL
        idx.update(over)
        return idx

    def start(self):
        net, d = self.net, self.order[self.phase]
        mine = self.view(self.index(), net.core)
        self.ids = {}
        for s in (1, -1) + ((2,) if self.direct[self.phase] else ()):
            self.ids[-s if s != 2 else 2] = net.send(mine, mine, net.chip(d, s))

    def take(self, s):
        net, d = self.net, self.order[self.phase]
        b = self.view(self.index(**{d: net.at(d, s)}), net.core)
        net.arrived(self.ids[s], b)
        if not self.direct[self.phase] and s == -self.forward:
            self.ids[2] = net.send(b, b, net.chip(d, self.forward))

    def step(self):
        for s in (-self.forward, self.forward, 2):
            self.take(s)
        self.phase += 1
        if self.phase < len(self.order):
            self.start()

    def share(self, s=None):
        d = self.order[self.phase]
        idx = self.index() if s is None else self.index(**{d: self.net.at(d, s)})
        b = self.view(idx, self.net.core)
        self.shared.append((self.net.send(b, b, self.net.partner()), idx))

    def get_shared(self):
        for i, idx in self.shared:
            self.net.arrived(i, self.view(idx, 1 - self.net.core))


def dot(a, b, ca=1, cb=0):
    return lax.dot_general(a, b, (((ca,), (cb,)), ((), ())), preferred_element_type=F32)


def splits(x):
    hi = x.astype(BF)
    rest = x - hi.astype(F32)
    mid = rest.astype(BF)
    return hi, mid, (rest - mid.astype(F32)).astype(BF)


def func_features(g):
    row = lax.broadcasted_iota(jnp.int32, g.shape, 0)
    ph = jnp.where((row >= 3) & (row != 6), g * TURN, 0.0)
    ex = g[6:7] * LOG2E
    c2 = g[0:1] * g[0:1] + g[1:2] * g[1:2] + g[2:3] * g[2:3]
    ee = jnp.where(row < 3, 2.0 * ex * g, jnp.where(row == 6, -ex, jnp.where(row == 7, LOG_S - ex * c2, 0.0)))
    hi, mid, lo = splits(jnp.concatenate([ph, ee], axis=0))
    return jnp.concatenate([hi, hi, hi, mid, mid, mid, lo, lo], axis=0)


def point_features(p):
    p0, p1, p2 = p
    row = lax.broadcasted_iota(jnp.int32, (8, p0.shape[1]), 0)
    rows = lambda *pairs: functools.reduce(lambda acc, rv: jnp.where(row == rv[0], rv[1], acc), pairs, jnp.zeros(row.shape, F32))
    ph = rows((3, p0), (4, p1), (5, p2), (7, 1.0))
    ee = rows((0, p0), (1, p1), (2, p2), (6, p0 * p0 + p1 * p1 + p2 * p2), (7, 1.0))
    zero = jnp.zeros_like(ph)
    out = []
    for parts in ([ph, zero], [zero, ee]):
        hi, mid, lo = splits(jnp.concatenate(parts, axis=0))
        out.append(jnp.concatenate([hi, mid, lo, hi, mid, lo, hi, mid], axis=0))
    return out


def basis(phase, exponent):
    r = phase - lax.round(phase, lax.RoundingMethod.TO_NEAREST_EVEN)
    z = jnp.abs(r) - 0.25
    y = z * z
    return (jnp.exp2(exponent) * (z * (((y + D2) * y + D1) * y + D0))).astype(BF)


def chunks():
    return [pl.ds(c, CHUNK) for c in range(0, GRID, CHUNK)]


def fused(
    occ, tri, cen, wav, exo, pha, pts, den, wts, src, out,
    O, T, G, par, FT, FR, PT, PP, phiR, phiC, B, rho, vk, Rb, H, A, S, A2,
    send_sem, recv_sem, local_sem,
):
    net = Net(send_sem, recv_sem)
    x, y, z, core = net.pos["x"], net.pos["y"], net.pos["z"], net.core
    local = [
        pltpu.make_async_copy(occ, O.at[x, y, z, core], local_sem.at[0]),
        pltpu.make_async_copy(tri, T.at[:, x, y], local_sem.at[1]),
    ]
    for c in local:
        c.start()
    par[...] = jnp.zeros_like(par)
    par[0:3, 0:64] = cen[...]
    par[3:6, 0:64] = wav[...]
    par[6:7, 0:64] = exo[...]
    par[7:8, 0:64] = pha[...]
    G[z, core, x, y] = par[...]
    barrier(net)
    for c in local:
        c.wait()

    gp = Gather(net, lambda i, c: G.at[i["z"], c, i["x"], i["y"]], "xyz", (1, 1, 1))
    go = [
        Gather(net, lambda i, c, p=p: O.at[i["x"], i["y"], i["z"], c, p], o, (1, 1, 0), f)
        for p, (o, f) in enumerate((("xyz", 1), ("yxz", -1), ("zxy", -1), ("zyx", -1)))
    ]
    gt = [Gather(net, lambda i, c, k=k: T.at[k, i["x"], i["y"]], o, (1, 0), -1) for k, o in enumerate(("xy", "yx"))]
    gp.start()
    for g in go + gt:
        g.start()

    for b in range(2):
        f = point_features([pts[i, b : b + 1, :] for i in range(3)])
        for i in range(2):
            PT[b, i] = f[i]
            PP[b, i] = f[i].T
    gp.step()
    for g in go + gt:
        g.step()
    gp.step()
    gp.share()

    def tile_features(zz, cc, xx):
        return func_features(jnp.concatenate([G[zz, cc, xx, i][:, :64] for i in range(4)], axis=1))

    for a in range(4):
        FR[a] = tile_features(z, core, a).T

    def rows(lo, hi):
        def body(i, _):
            b, a = i // 4, i % 4
            for sl in chunks():
                phiR[b, a, :, sl] = basis(dot(FR[a], PT[b, 0, :, sl]), dot(FR[a], PT[b, 1, :, sl]))
            return 0

        lax.fori_loop(lo, hi, body, 0)

    def cols(lo, hi):
        def body(i, _):
            b, j = i // 8, i % 8
            f = FT[src[b, 0, j] * 2 + j % 2]
            for sl in chunks():
                phiC[b, j, sl, :] = basis(dot(PP[b, 0, sl], f), dot(PP[b, 1, sl], f))
            return 0

        lax.fori_loop(lo, hi, body, 0)

    rows(0, 2)
    for g in go:
        g.step()
        g.share()
    rows(2, 5)
    for s in (1, -1, 2):
        gp.take(s)
        gp.share(s)
    rows(5, 8)
    for g in go:
        g.take(-g.forward)
        g.share(-g.forward)
    for g in gt:
        g.take(-g.forward)
    gp.get_shared()

    def all_features(t, _):
        FT[t] = tile_features(t // 8, (t // 4) % 2, t % 4)
        return 0

    lax.fori_loop(0, 32, all_features, 0)
    cols(0, 5)
    for g in go:
        g.take(g.forward)
        g.share(g.forward)
    cols(5, 16)
    for g in go:
        g.take(2)
        g.share(2)
    for g in go:
        g.get_shared()

    def half(i, _):
        b, a = i // 4, i % 4
        o = []
        for j in range(2):
            s = src[b, 0, 2 * a + j]
            o.append(O[s // 4, s % 4, 2 * j : 2 * j + 2].reshape(256, 512))
        for sl in chunks():
            B[i, sl, :] = (dot(phiC[b, 2 * a, sl, :], o[0]) + dot(phiC[b, 2 * a + 1, sl, :], o[1])).astype(BF)
        return 0

    rho[...] = jnp.zeros_like(rho)

    def densities(i):
        b, a = i // 4, i % 4
        factors = jnp.concatenate([T[0, a].reshape(256, 512), T[1, a].reshape(256, 512)], axis=0)
        for sl in chunks():
            cc = dot(factors, B[i, sl, :], 1, 1)
            phi = phiR[b, a, :, sl].astype(F32)
            for k in range(2):
                part = cc[k * 256 : (k + 1) * 256] * phi
                rho[b, k : k + 1, sl] += jnp.sum(part, axis=0, keepdims=True)

    def both(i, _):
        densities(i - 4)
        half(i, 0)
        return 0

    def last(i, _):
        densities(i)
        return 0

    def in_twos(step, lo, hi):
        def body(i, _):
            step(2 * i, 0)
            step(2 * i + 1, 0)
            return 0

        lax.fori_loop(lo // 2, hi // 2, body, 0)

    in_twos(half, 0, 4)
    for g in gt:
        g.take(g.forward)
        g.take(2)
    in_twos(both, 4, 8)
    in_twos(last, 4, 8)
    for b in range(2):
        f = wts[b : b + 1, :] * (-(4.0 / 9.0) * EXCHANGE_COEF * jnp.exp(-(2.0 / 3.0) * jnp.log(den[b : b + 1, :])))
        for k in range(2):
            vk[b, k : k + 1, :] = f * rho[b, k : k + 1, :]

    def tile(k, a):
        acc = None
        for b in range(2):
            sc = (phiR[b, a].astype(F32) * vk[b, k : k + 1, :]).astype(BF)
            d = dot(sc, B[b * 4 + a])
            acc = d if acc is None else acc + d
        Rb[k, a] = acc.astype(BF).reshape(4, 64, 512)

    dims = ("x", "y")

    def chunk(k, c, half=FULL):
        return Rb.at[0, c, half] if k == 0 else Rb.at[1, half, c]

    lows, highs = pl.ds(0, 2), pl.ds(2, 2)
    ids = [{}, {}]

    def opposite(k):
        d = dims[k]
        c = net.at(d, 2)
        ids[k]["h0"] = net.send(chunk(k, c, lows), H.at[k, 0], net.chip(d, 1))
        ids[k]["h1"] = net.send(chunk(k, c, highs), H.at[k, 1], net.chip(d, -1))

    def own_halves(k):
        d = dims[k]
        for n, (s, hs, part) in enumerate(((1, highs, 1), (-1, lows, 0))):
            ids[k][f"o{n}"] = net.send(chunk(k, net.at(d, s), hs), A.at[k, n, pl.ds(2 * part, 2)], net.chip(d, s))

    def summed_halves(k):
        d = dims[k]
        for n, (s, hs, part) in enumerate(((1, lows, 0), (-1, highs, 1))):
            net.arrived(ids[k][f"h{n}"], H.at[k, n])
            piece = chunk(k, net.at(d, s), hs)
            piece[...] = (piece[...].astype(F32) + H[k, n].astype(F32)).astype(BF)
            ids[k][f"a{n}"] = net.send(piece, A.at[k, n, pl.ds(2 * part, 2)], net.chip(d, s))

    def second(k):
        d, e = dims[k], dims[1 - k]
        for n, part in enumerate((0, 1)):
            net.arrived(ids[k][f"o{n}"], A.at[k, n, pl.ds(2 - 2 * part, 2)])
            net.arrived(ids[k][f"a{n}"], A.at[k, n, pl.ds(2 * part, 2)])
        total = chunk(k, net.pos[d])[...].astype(F32) + A[k, 0].astype(F32) + A[k, 1].astype(F32)
        S[k] = total.astype(BF)
        for n, s in enumerate((2, 1, -1)):
            ids[k][f"s{n}"] = net.send(S.at[k, net.at(e, s)], A2.at[k, n], net.chip(e, s))

    def finish(k):
        total = S[k, net.pos[dims[1 - k]]].astype(F32)
        for n in range(3):
            net.arrived(ids[k][f"s{n}"], A2.at[k, n])
            total = total + A2[k, n].astype(F32)
        out[:, k, :] = total

    def tiles_1(a, _):
        tile(1, a)
        return 0

    in_twos(tiles_1, 0, 4)
    opposite(1)
    own_halves(1)
    tile(0, net.at("x", 2))
    opposite(0)
    tile(0, net.at("x", 1))
    tile(0, net.at("x", -1))
    own_halves(0)
    summed_halves(1)
    summed_halves(0)
    tile(0, net.pos["x"])
    second(1)
    second(0)
    finish(1)
    finish(0)
    net.drain()


SEMS = 140


def per_device(tri, occ, cen, exo, wav, pha, pts, den, wts, src):
    vmem, hbm = pl.BlockSpec(memory_space=pltpu.VMEM), pl.BlockSpec(memory_space=pl.ANY)
    return pl.pallas_call(
        fused,
        out_shape=jax.ShapeDtypeStruct((64, 2, 512), F32),
        in_specs=[hbm, hbm] + [vmem] * 7 + [pl.BlockSpec(memory_space=pltpu.SMEM)],
        out_specs=vmem,
        scratch_shapes=[
            pltpu.VMEM((4, 4, 4, 2, 4, 16, 512), BF),
            pltpu.VMEM((2, 4, 4, 64, 512), BF),
            pltpu.VMEM((4, 2, 4, 4, 8, 128), F32),
            pltpu.VMEM((8, 128), F32),
            pltpu.VMEM((32, 128, 256), BF),
            pltpu.VMEM((4, 256, 128), BF),
            pltpu.VMEM((2, 2, 128, GRID), BF),
            pltpu.VMEM((2, 2, GRID, 128), BF),
            pltpu.VMEM((2, 4, 256, GRID), BF),
            pltpu.VMEM((2, 8, GRID, 256), BF),
            pltpu.VMEM((8, GRID, 512), BF),
            pltpu.VMEM((2, 2, GRID), F32),
            pltpu.VMEM((2, 2, GRID), F32),
            pltpu.VMEM((2, 4, 4, 64, 512), BF),
            pltpu.VMEM((2, 2, 2, 64, 512), BF),
            pltpu.VMEM((2, 2, 4, 64, 512), BF),
            pltpu.VMEM((2, 4, 64, 512), BF),
            pltpu.VMEM((2, 3, 64, 512), BF),
            pltpu.SemaphoreType.DMA((SEMS,)),
            pltpu.SemaphoreType.DMA((SEMS,)),
            pltpu.SemaphoreType.DMA((2,)),
        ],
        compiler_params=pltpu.CompilerParams(collective_id=0, has_side_effects=True, vmem_limit_bytes=62 * 2**20),
        name="fused",
    )(occ.reshape(4, 16, 512), tri, cen, wav, exo.reshape(1, 64), pha.reshape(1, 64), pts.transpose(1, 0, 2), den, wts, src.transpose(0, 2, 1))


def solution(mesh):
    both = ("row", "col")
    in_specs = (
        P(None, both, None),
        P(("col", "row"), None),
        P(None, both),
        P(both),
        P(None, both),
        P(both),
        P(both, None, None),
        P(both, None),
        P(both, None),
        P(both, None, None),
    )
    return jax.shard_map(per_device, mesh=mesh, in_specs=in_specs, out_specs=P(both, None, None), check_vma=False)
```

```python
import functools
import math

import jax
import jax.numpy as jnp
from jax import lax
from jax.experimental import pallas as pl
from jax.experimental.pallas import tpu as pltpu
from jax.sharding import PartitionSpec as P

BF = jnp.bfloat16
F32 = jnp.float32
MESH = pl.DeviceIdType.MESH
FULL = slice(None)
EXCHANGE_COEF = 0.75 * (3.0 / 3.141592653589793) ** (1.0 / 3.0)
S0, S1, S2, S3 = 6.283164044302474, -41.33714237110029, 81.34076888766828, -70.99343327209985
D0, D1, D2 = S0 / S3, S1 / S3, S2 / S3
LOG_S = math.log2(-S3)
LOG2E = math.log2(math.e)
TURN = 1.0 / (2.0 * math.pi)
GRID = 1024
CHUNK = 256


class Net:
    def __init__(self, send_sem, recv_sem):
        self.row, self.col = lax.axis_index("row"), lax.axis_index("col")
        self.pos = {"x": self.col // 4, "y": self.col % 4, "z": self.row // 2}
        self.core = self.row % 2
        self.send_sem, self.recv_sem = send_sem, recv_sem
        self.count = 0
        self.sent = []

    def at(self, dim, step):
        return lax.rem(self.pos[dim] + (step + 4), 4)

    def chip(self, dim, step):
        p = dict(self.pos)
        p[dim] = self.at(dim, step)
        return (p["z"] * 2 + self.core, p["x"] * 4 + p["y"])

    def partner(self):
        return (self.row + 1 - 2 * self.core, self.col)

    def copy(self, i, src, dst, device):
        return pltpu.make_async_remote_copy(
            src_ref=src,
            dst_ref=dst,
            send_sem=self.send_sem.at[i],
            recv_sem=self.recv_sem.at[i],
            device_id=device,
            device_id_type=MESH,
        )

    def send(self, src, dst, device):
        i = self.count
        self.count += 1
        c = self.copy(i, src, dst, device)
        c.start()
        self.sent.append(c)
        return i

    def arrived(self, i, dst):
        self.copy(i, dst, dst, self.partner()).wait_recv()

    def drain(self):
        for c in self.sent:
            c.wait_send()
        self.sent = []


def barrier(net):
    sem = pltpu.get_barrier_semaphore()
    peers = [net.partner()] + [net.chip(d, s) for d in "xyz" for s in (1, -1, 2)]
    for p in peers:
        pl.semaphore_signal(sem, inc=1, device_id=p, device_id_type=MESH)
    pl.semaphore_wait(sem, len(peers))


class Gather:
    def __init__(self, net, view, order, direct, forward=1):
        self.net, self.view, self.order, self.direct, self.forward = net, view, order, direct, forward
        self.phase = 0
        self.shared = []

    def index(self, **over):
        idx = dict(self.net.pos)
        for d in self.order[: self.phase]:
            idx[d] = FULL
        idx.update(over)
        return idx

    def start(self):
        net, d = self.net, self.order[self.phase]
        mine = self.view(self.index(), net.core)
        self.ids = {}
        for s in (1, -1) + ((2,) if self.direct[self.phase] else ()):
            self.ids[-s if s != 2 else 2] = net.send(mine, mine, net.chip(d, s))

    def take(self, s):
        net, d = self.net, self.order[self.phase]
        b = self.view(self.index(**{d: net.at(d, s)}), net.core)
        net.arrived(self.ids[s], b)
        if not self.direct[self.phase] and s == -self.forward:
            self.ids[2] = net.send(b, b, net.chip(d, self.forward))

    def step(self):
        for s in (-self.forward, self.forward, 2):
            self.take(s)
        self.phase += 1
        if self.phase < len(self.order):
            self.start()

    def share(self, s=None):
        d = self.order[self.phase]
        idx = self.index() if s is None else self.index(**{d: self.net.at(d, s)})
        b = self.view(idx, self.net.core)
        self.shared.append((self.net.send(b, b, self.net.partner()), idx))

    def get_shared(self):
        for i, idx in self.shared:
            self.net.arrived(i, self.view(idx, 1 - self.net.core))


def dot(a, b, ca=1, cb=0):
    return lax.dot_general(a, b, (((ca,), (cb,)), ((), ())), preferred_element_type=F32)


def splits(x):
    hi = x.astype(BF)
    rest = x - hi.astype(F32)
    mid = rest.astype(BF)
    return hi, mid, (rest - mid.astype(F32)).astype(BF)


def func_features(g):
    row = lax.broadcasted_iota(jnp.int32, g.shape, 0)
    ph = jnp.where((row >= 3) & (row != 6), g * TURN, 0.0)
    ex = g[6:7] * LOG2E
    c2 = g[0:1] * g[0:1] + g[1:2] * g[1:2] + g[2:3] * g[2:3]
    ee = jnp.where(row < 3, 2.0 * ex * g, jnp.where(row == 6, -ex, jnp.where(row == 7, LOG_S - ex * c2, 0.0)))
    hi, mid, lo = splits(jnp.concatenate([ph, ee], axis=0))
    return jnp.concatenate([hi, hi, hi, mid, mid, mid, lo, lo], axis=0)


def point_features(p):
    p0, p1, p2 = p
    row = lax.broadcasted_iota(jnp.int32, (8, p0.shape[1]), 0)
    rows = lambda *pairs: functools.reduce(lambda acc, rv: jnp.where(row == rv[0], rv[1], acc), pairs, jnp.zeros(row.shape, F32))
    ph = rows((3, p0), (4, p1), (5, p2), (7, 1.0))
    ee = rows((0, p0), (1, p1), (2, p2), (6, p0 * p0 + p1 * p1 + p2 * p2), (7, 1.0))
    zero = jnp.zeros_like(ph)
    out = []
    for parts in ([ph, zero], [zero, ee]):
        hi, mid, lo = splits(jnp.concatenate(parts, axis=0))
        out.append(jnp.concatenate([hi, mid, lo, hi, mid, lo, hi, mid], axis=0))
    return out


def basis(phase, exponent):
    r = phase - lax.round(phase, lax.RoundingMethod.TO_NEAREST_EVEN)
    z = jnp.abs(r) - 0.25
    y = z * z
    return (jnp.exp2(exponent) * (z * (((y + D2) * y + D1) * y + D0))).astype(BF)


def chunks():
    return [pl.ds(c, CHUNK) for c in range(0, GRID, CHUNK)]


def fused(
    occ, tri, cen, wav, exo, pha, pts, den, wts, src, out,
    O, T, G, par, FT, FR, PT, PP, phiR, phiC, B, rho, vk, Rb, H, A, S, A2,
    send_sem, recv_sem, local_sem,
):
    net = Net(send_sem, recv_sem)
    x, y, z, core = net.pos["x"], net.pos["y"], net.pos["z"], net.core
    local = [
        pltpu.make_async_copy(occ, O.at[x, y, z, core], local_sem.at[0]),
        pltpu.make_async_copy(tri, T.at[:, x, y], local_sem.at[1]),
    ]
    for c in local:
        c.start()
    par[...] = jnp.zeros_like(par)
    par[0:3, 0:64] = cen[...]
    par[3:6, 0:64] = wav[...]
    par[6:7, 0:64] = exo[...]
    par[7:8, 0:64] = pha[...]
    G[z, core, x, y] = par[...]
    barrier(net)
    for c in local:
        c.wait()

    gp = Gather(net, lambda i, c: G.at[i["z"], c, i["x"], i["y"]], "xyz", (1, 1, 1))
    go = [
        Gather(net, lambda i, c, p=p: O.at[i["x"], i["y"], i["z"], c, p], o, (1, 1, 0), f)
        for p, (o, f) in enumerate((("xyz", 1), ("yxz", -1), ("zxy", -1), ("zyx", -1)))
    ]
    gt = [Gather(net, lambda i, c, k=k: T.at[k, i["x"], i["y"]], o, (1, 0), -1) for k, o in enumerate(("xy", "yx"))]
    gp.start()
    for g in go + gt:
        g.start()

    for b in range(2):
        f = point_features([pts[i, b : b + 1, :] for i in range(3)])
        for i in range(2):
            PT[b, i] = f[i]
            PP[b, i] = f[i].T
    gp.step()
    for g in go + gt:
        g.step()
    gp.step()
    gp.share()

    def tile_features(zz, cc, xx):
        return func_features(jnp.concatenate([G[zz, cc, xx, i][:, :64] for i in range(4)], axis=1))

    for a in range(4):
        FR[a] = tile_features(z, core, a).T

    def rows(lo, hi):
        def body(i, _):
            b, a = i // 4, i % 4
            for sl in chunks():
                phiR[b, a, :, sl] = basis(dot(FR[a], PT[b, 0, :, sl]), dot(FR[a], PT[b, 1, :, sl]))
            return 0

        lax.fori_loop(lo, hi, body, 0)

    def cols(lo, hi):
        def body(i, _):
            b, j = i // 8, i % 8
            f = FT[src[b, 0, j] * 2 + j % 2]
            for sl in chunks():
                phiC[b, j, sl, :] = basis(dot(PP[b, 0, sl], f), dot(PP[b, 1, sl], f))
            return 0

        lax.fori_loop(lo, hi, body, 0)

    rows(0, 2)
    for g in go:
        g.step()
        g.share()
    rows(2, 5)
    for s in (1, -1, 2):
        gp.take(s)
        gp.share(s)
    rows(5, 8)
    for g in go:
        g.take(-g.forward)
        g.share(-g.forward)
    for g in gt:
        g.take(-g.forward)
    gp.get_shared()

    def all_features(t, _):
        FT[t] = tile_features(t // 8, (t // 4) % 2, t % 4)
        return 0

    lax.fori_loop(0, 32, all_features, 0)
    cols(0, 5)
    for g in go:
        g.take(g.forward)
        g.share(g.forward)
    cols(5, 16)
    for g in go:
        g.take(2)
        g.share(2)
    for g in go:
        g.get_shared()

    def half(i, _):
        b, a = i // 4, i % 4
        o = []
        for j in range(2):
            s = src[b, 0, 2 * a + j]
            o.append(O[s // 4, s % 4, 2 * j : 2 * j + 2].reshape(256, 512))
        for sl in chunks():
            B[i, sl, :] = (dot(phiC[b, 2 * a, sl, :], o[0]) + dot(phiC[b, 2 * a + 1, sl, :], o[1])).astype(BF)
        return 0

    rho[...] = jnp.zeros_like(rho)

    def densities(i):
        b, a = i // 4, i % 4
        factors = jnp.concatenate([T[0, a].reshape(256, 512), T[1, a].reshape(256, 512)], axis=0)
        for sl in chunks():
            cc = dot(factors, B[i, sl, :], 1, 1)
            phi = phiR[b, a, :, sl].astype(F32)
            for k in range(2):
                part = cc[k * 256 : (k + 1) * 256] * phi
                rho[b, k : k + 1, sl] += jnp.sum(part, axis=0, keepdims=True)

    def both(i, _):
        densities(i - 4)
        half(i, 0)
        return 0

    def last(i, _):
        densities(i)
        return 0

    def in_fours(step, lo):
        def body(i, _):
            for j in range(4):
                step(4 * i + j, 0)
            return 0

        lax.fori_loop(lo // 4, lo // 4 + 1, body, 0)

    in_fours(half, 0)
    for g in gt:
        g.take(g.forward)
        g.take(2)
    in_fours(both, 4)
    in_fours(last, 4)
    for b in range(2):
        f = wts[b : b + 1, :] * (-(4.0 / 9.0) * EXCHANGE_COEF * jnp.exp(-(2.0 / 3.0) * jnp.log(den[b : b + 1, :])))
        for k in range(2):
            vk[b, k : k + 1, :] = f * rho[b, k : k + 1, :]

    def tile(k, a):
        acc = None
        for b in range(2):
            sc = (phiR[b, a].astype(F32) * vk[b, k : k + 1, :]).astype(BF)
            d = dot(sc, B[b * 4 + a])
            acc = d if acc is None else acc + d
        Rb[k, a] = acc.astype(BF).reshape(4, 64, 512)

    dims = ("x", "y")

    def chunk(k, c, half=FULL):
        return Rb.at[0, c, half] if k == 0 else Rb.at[1, half, c]

    lows, highs = pl.ds(0, 2), pl.ds(2, 2)
    ids = [{}, {}]

    def opposite(k):
        d = dims[k]
        c = net.at(d, 2)
        ids[k]["h0"] = net.send(chunk(k, c, lows), H.at[k, 0], net.chip(d, 1))
        ids[k]["h1"] = net.send(chunk(k, c, highs), H.at[k, 1], net.chip(d, -1))

    def own_halves(k):
        d = dims[k]
        for n, (s, hs, part) in enumerate(((1, highs, 1), (-1, lows, 0))):
            ids[k][f"o{n}"] = net.send(chunk(k, net.at(d, s), hs), A.at[k, n, pl.ds(2 * part, 2)], net.chip(d, s))

    def summed_halves(k):
        d = dims[k]
        for n, (s, hs, part) in enumerate(((1, lows, 0), (-1, highs, 1))):
            net.arrived(ids[k][f"h{n}"], H.at[k, n])
            piece = chunk(k, net.at(d, s), hs)
            piece[...] = (piece[...].astype(F32) + H[k, n].astype(F32)).astype(BF)
            ids[k][f"a{n}"] = net.send(piece, A.at[k, n, pl.ds(2 * part, 2)], net.chip(d, s))

    def second(k):
        d, e = dims[k], dims[1 - k]
        for n, part in enumerate((0, 1)):
            net.arrived(ids[k][f"o{n}"], A.at[k, n, pl.ds(2 - 2 * part, 2)])
            net.arrived(ids[k][f"a{n}"], A.at[k, n, pl.ds(2 * part, 2)])
        total = chunk(k, net.pos[d])[...].astype(F32) + A[k, 0].astype(F32) + A[k, 1].astype(F32)
        S[k] = total.astype(BF)
        for n, s in enumerate((2, 1, -1)):
            ids[k][f"s{n}"] = net.send(S.at[k, net.at(e, s)], A2.at[k, n], net.chip(e, s))

    def finish(k):
        total = S[k, net.pos[dims[1 - k]]].astype(F32)
        for n in range(3):
            net.arrived(ids[k][f"s{n}"], A2.at[k, n])
            total = total + A2[k, n].astype(F32)
        out[:, k, :] = total

    def tiles_1(a, _):
        tile(1, a)
        return 0

    in_fours(tiles_1, 0)
    opposite(1)
    own_halves(1)
    tile(0, net.at("x", 2))
    opposite(0)
    tile(0, net.at("x", 1))
    tile(0, net.at("x", -1))
    own_halves(0)
    summed_halves(1)
    summed_halves(0)
    tile(0, net.pos["x"])
    second(1)
    second(0)
    finish(1)
    finish(0)
    net.drain()


SEMS = 140


def per_device(tri, occ, cen, exo, wav, pha, pts, den, wts, src):
    vmem, hbm = pl.BlockSpec(memory_space=pltpu.VMEM), pl.BlockSpec(memory_space=pl.ANY)
    return pl.pallas_call(
        fused,
        out_shape=jax.ShapeDtypeStruct((64, 2, 512), F32),
        in_specs=[hbm, hbm] + [vmem] * 7 + [pl.BlockSpec(memory_space=pltpu.SMEM)],
        out_specs=vmem,
        scratch_shapes=[
            pltpu.VMEM((4, 4, 4, 2, 4, 16, 512), BF),
            pltpu.VMEM((2, 4, 4, 64, 512), BF),
            pltpu.VMEM((4, 2, 4, 4, 8, 128), F32),
            pltpu.VMEM((8, 128), F32),
            pltpu.VMEM((32, 128, 256), BF),
            pltpu.VMEM((4, 256, 128), BF),
            pltpu.VMEM((2, 2, 128, GRID), BF),
            pltpu.VMEM((2, 2, GRID, 128), BF),
            pltpu.VMEM((2, 4, 256, GRID), BF),
            pltpu.VMEM((2, 8, GRID, 256), BF),
            pltpu.VMEM((8, GRID, 512), BF),
            pltpu.VMEM((2, 2, GRID), F32),
            pltpu.VMEM((2, 2, GRID), F32),
            pltpu.VMEM((2, 4, 4, 64, 512), BF),
            pltpu.VMEM((2, 2, 2, 64, 512), BF),
            pltpu.VMEM((2, 2, 4, 64, 512), BF),
            pltpu.VMEM((2, 4, 64, 512), BF),
            pltpu.VMEM((2, 3, 64, 512), BF),
            pltpu.SemaphoreType.DMA((SEMS,)),
            pltpu.SemaphoreType.DMA((SEMS,)),
            pltpu.SemaphoreType.DMA((2,)),
        ],
        compiler_params=pltpu.CompilerParams(collective_id=0, has_side_effects=True, vmem_limit_bytes=62 * 2**20),
        name="fused",
    )(occ.reshape(4, 16, 512), tri, cen, wav, exo.reshape(1, 64), pha.reshape(1, 64), pts.transpose(1, 0, 2), den, wts, src.transpose(0, 2, 1))


def solution(mesh):
    both = ("row", "col")
    in_specs = (
        P(None, both, None),
        P(("col", "row"), None),
        P(None, both),
        P(both),
        P(None, both),
        P(both),
        P(both, None, None),
        P(both, None),
        P(both, None),
        P(both, None, None),
    )
    return jax.shard_map(per_device, mesh=mesh, in_specs=in_specs, out_specs=P(both, None, None), check_vma=False)
```
